256 devices in a mesh: blk: 128 (over z_lo, y, x, core), rep: 2 (over z_hi).
Axes of the slice: x: 4, y: 4, z: 8 (z_hi: 2, z_lo: 4; z = z_hi * 4 + z_lo), core: 2. Of those that a mesh axis runs over, the one named last changes fastest.
Arguments:
- load_coef: bfloat16 [256, 2049, 256], P('blk', None, 'rep'), parts along dimension 2, may hold values from -0.29882812 to 0.29882812
- legendre: bfloat16 [256, 2049, 1024], P('blk'), may hold values from -0.125 to 0.125
- slab_orders: int32 [256], replicated, may hold values from 0 to 1023, as said below
- cycle_rows: int32 [1024], replicated, may hold values from 0 to 1023, each once
Outputs:
- potential: bfloat16 [1024, 128, 4096], P('blk', 'rep'), parts along dimension 1
- energy: float32 [128], P('rep'), parts along dimension 0
The draws below stay inside these ranges and needn't reach their ends.
There are 2 independent parts, one for each index of `rep`. The reference program is written for one: setup_inputs(seed, part) draws one part's arguments, and reference() takes and returns one part's arrays. A program takes and returns all parts, laid end to end along the dimension named above; an argument that names none is the same for every part. Nothing has to cross between parts.
Inputs may be any that keep to these rules, and one draw needn't show every extreme that they name: `slab_orders`: values are distinct and below (2048) / 2. `cycle_rows`: each cycle appears once.
All inputs are finite; a program needn't handle non-finite values.
Results may differ from the reference program's by a relative error of at most 0.0055.
Values may be sent and summed in bfloat16 or wider, within the bound.
A program may use at most 128 MiB of HBM per device.

```python
import math
import jax
import jax.numpy as jnp
from jax import lax

DEGREE = 2047
NLAT = 1024
NLON = 4096
FIELDS = 64
SLAB = 2049
PAIRS = 256


def draw_slab_orders(key, part):
    return jax.random.permutation(key, (DEGREE + 1) // 2)[:PAIRS].astype(jnp.int32)


def levels(key, dims, shards, smallest, top_value):
    loudness = 1.0
    for axis_at, blocks in shards:
        draws = jax.random.uniform(jax.random.fold_in(jax.random.fold_in(key, 6), axis_at), (blocks,), jnp.float32, smallest / len(shards), top_value / len(shards))
        loudness = loudness * jnp.repeat(jnp.exp(draws), dims[axis_at] // blocks).reshape((-1,) + (1,) * (len(dims) - 1 - axis_at))
    return loudness


def scatter_about(key, dims, scale, limit, pieces=(), kind=jnp.bfloat16):
    values = jax.random.normal(key, dims, jnp.float32) * scale
    if len(pieces) > 0:
        values = levels(key, dims, pieces, -0.22, 0.18) * values
    return jnp.clip(values, min=-limit, max=limit).astype(kind)


def setup_inputs(seed: int = 0, part: int = 0) -> dict:
    streams_of = jax.random.split(jax.random.key(seed), 5)
    part_splits = jax.random.split(jax.random.fold_in(streams_of[4], part), 5)
    load_coef = scatter_about(part_splits[0], (PAIRS, SLAB, 2 * FIELDS), 0.05, 0.29882812, ((0, 128),))
    legendre = scatter_about(streams_of[1], (PAIRS, SLAB, NLAT), SLAB ** -0.5, 0.125, ((0, 128),))
    slab_orders = draw_slab_orders(jax.random.fold_in(streams_of[4], 71), part)
    cycle_rows = jax.random.permutation(streams_of[3], NLAT).astype(jnp.int32)
    return {"load_coef": load_coef, "legendre": legendre, "slab_orders": slab_orders, "cycle_rows": cycle_rows}


def basis_table(orders):
    longitude_ids = jnp.arange(NLON, dtype=jnp.int32)
    phase_ids = (orders[:, None] * longitude_ids[None, :]) % NLON
    angles = phase_ids.astype(jnp.float32) * (2.0 * math.pi / NLON)
    factor = jnp.where(orders == 0, 1.0, 2.0).astype(jnp.float32)[:, None]
    return (factor * jnp.cos(angles)).astype(jnp.bfloat16), (-factor * jnp.sin(angles)).astype(jnp.bfloat16)


def reference(load_coef, legendre, slab_orders, cycle_rows):
    slab_rows = DEGREE + 2
    row_ids = jnp.arange(slab_rows, dtype=jnp.int32)

    def synthesize(pair_args):
        pair_coef, pair_table, low_order = pair_args
        in_lower = (row_ids < slab_rows - 1 - low_order)[:, None]
        nothing = jnp.zeros_like(pair_coef)
        stacked = jnp.concatenate([jnp.where(in_lower, pair_coef, nothing), jnp.where(in_lower, nothing, pair_coef)], axis=1)
        return lax.dot_general(stacked, pair_table, (((0,), (0,)), ((), ())), preferred_element_type=jnp.float32).astype(jnp.bfloat16)

    spectra = lax.map(synthesize, (load_coef, legendre, slab_orders))
    spectra = spectra.reshape(PAIRS, 4, FIELDS, NLAT)
    cos_lower, sin_lower = basis_table(slab_orders.astype(jnp.int32))
    cos_upper, sin_upper = basis_table((DEGREE - slab_orders).astype(jnp.int32))
    basis = jnp.stack([cos_lower, sin_lower, cos_upper, sin_upper], axis=1).reshape(PAIRS * 4, NLON)

    def per_field(field_index):
        rows = spectra[:, :, field_index, :].reshape(PAIRS * 4, NLAT)
        wave = lax.dot_general(rows, basis, (((0,), (0,)), ((), ())), preferred_element_type=jnp.float32)
        energy = jnp.sum(wave * wave) / (NLAT * NLON)
        return wave[cycle_rows].astype(jnp.bfloat16), energy

    potential, energy = lax.map(per_field, jnp.arange(FIELDS, dtype=jnp.int32))
    return jnp.transpose(potential, (1, 0, 2)), energy
```

```python
import math

import jax
import jax.numpy as jnp
from jax import lax
from jax.experimental import pallas as pl
from jax.experimental.pallas import tpu as pltpu
from jax.sharding import PartitionSpec as P

NLON = 4096
BLK = "blk"
N = 128
MESH = pl.DeviceIdType.MESH


def basis_rows(frequency):
    coarse_ids = jnp.arange(NLON // 64, dtype=jnp.int32) * 64
    fine_ids = jnp.arange(64, dtype=jnp.int32)
    scale = 2.0 * math.pi / NLON
    coarse_angles = (frequency[:, None] * coarse_ids[None, :] % NLON).astype(jnp.float32) * scale
    fine_angles = (frequency[:, None] * fine_ids[None, :] % NLON).astype(jnp.float32) * scale
    cos_coarse = jnp.cos(coarse_angles)[:, :, None]
    sin_coarse = jnp.sin(coarse_angles)[:, :, None]
    cos_fine = jnp.cos(fine_angles)[:, None, :]
    sin_fine = jnp.sin(fine_angles)[:, None, :]
    cosine = (cos_coarse * cos_fine - sin_coarse * sin_fine).reshape(frequency.shape[0], NLON)
    sine = (sin_coarse * cos_fine + cos_coarse * sin_fine).reshape(frequency.shape[0], NLON)
    factor = jnp.where(frequency == 0, 1.0, 2.0).astype(jnp.float32)[:, None]
    return ((factor * cosine).astype(jnp.bfloat16), (-factor * sine).astype(jnp.bfloat16))


def fourier(received, low_orders, degree):
    cos_lower, sin_lower = basis_rows(low_orders)
    cos_upper, sin_upper = basis_rows(degree - low_orders)
    fourier_basis = jnp.stack([cos_lower, sin_lower, cos_upper, sin_upper], axis=1)
    return jnp.einsum("rnsf,nsk->rfk", received, fourier_basis, preferred_element_type=jnp.float32)


def exchange_kernel(x_ref, o_ref, send_sem, recv_sem):
    me = lax.axis_index(BLK)
    barrier = pltpu.get_barrier_semaphore()

    def greet(step, carry):
        pl.semaphore_signal(
            barrier, inc=1, device_id={BLK: (me + step) % N}, device_id_type=MESH
        )
        return carry

    lax.fori_loop(1, N, greet, 0)
    pl.semaphore_wait(barrier, N - 1)

    def send(step, carry):
        target = (me + (step % 4) * 32 + step // 4) % N
        pltpu.make_async_remote_copy(
            src_ref=x_ref.at[target],
            dst_ref=o_ref.at[me],
            send_sem=send_sem,
            recv_sem=recv_sem,
            device_id={BLK: target},
            device_id_type=MESH,
        ).start()
        return carry

    lax.fori_loop(1, N, send, 0)
    o_ref[me] = x_ref[me]
    everything = pltpu.make_async_remote_copy(
        src_ref=x_ref.at[pl.ds(0, N - 1)],
        dst_ref=o_ref.at[pl.ds(0, N - 1)],
        send_sem=send_sem,
        recv_sem=recv_sem,
        device_id={BLK: (me + 1) % N},
        device_id_type=MESH,
    )
    everything.wait()


def exchange(x):
    return pl.pallas_call(
        exchange_kernel,
        out_shape=jax.ShapeDtypeStruct(x.shape, x.dtype),
        in_specs=[pl.BlockSpec(memory_space=pltpu.VMEM)],
        out_specs=pl.BlockSpec(memory_space=pltpu.VMEM),
        scratch_shapes=[pltpu.SemaphoreType.DMA, pltpu.SemaphoreType.DMA],
        name="exchange",
        compiler_params=pltpu.CompilerParams(collective_id=0, has_side_effects=True),
    )(x)


def shards(load_coef, legendre, slab_orders, cycle_rows):
    blocks = lax.axis_size(BLK)
    position = lax.axis_index(BLK)
    pair_count = load_coef.shape[0]
    slab_rows = load_coef.shape[1]
    fields = load_coef.shape[2] // 2
    lat_count = legendre.shape[2]
    degree = slab_rows - 2
    my_orders = lax.dynamic_slice_in_dim(slab_orders, position * pair_count, pair_count)
    row_ids = jnp.arange(slab_rows, dtype=jnp.int32)
    spectra = []
    for pair_index in range(pair_count):
        in_lower = (row_ids < slab_rows - 1 - my_orders[pair_index])[:, None]
        pair_coef = load_coef[pair_index]
        nothing = jnp.zeros_like(pair_coef)
        stacked = jnp.concatenate(
            [jnp.where(in_lower, pair_coef, nothing), jnp.where(in_lower, nothing, pair_coef)],
            axis=1,
        )
        spectra.append(
            lax.dot_general(
                legendre[pair_index],
                stacked,
                (((0,), (0,)), ((), ())),
                preferred_element_type=jnp.float32,
            ).astype(jnp.bfloat16)
        )
    spectra = jnp.stack(spectra, axis=1).reshape(lat_count, pair_count, 4, fields)
    spectra = jnp.take(spectra, cycle_rows, axis=0)
    all_orders = slab_orders.reshape(blocks, pair_count)
    rows = lat_count // blocks
    received = exchange(spectra.reshape(blocks, 2 * rows, -1))
    received = received.reshape(blocks, rows, pair_count, 4, fields)
    received = received.transpose(1, 0, 2, 3, 4).reshape(rows, blocks * pair_count, 4, fields)
    cycle_grid = fourier(received, low_orders=all_orders.reshape(-1), degree=degree)
    partial_energy = jnp.sum(cycle_grid * cycle_grid, axis=(0, 2))
    summed = lax.psum(partial_energy, BLK)
    energy = summed / (lat_count * NLON)
    return (cycle_grid.astype(jnp.bfloat16), energy)


def solution(mesh):
    in_specs = (P(BLK, None, "rep"), P(BLK, None, None), P(), P())
    out_specs = (P(BLK, "rep", None), P("rep"))
    return jax.shard_map(
        shards, mesh=mesh, in_specs=in_specs, out_specs=out_specs, check_vma=False
    )
```

```python
import functools
import math

import jax
import jax.numpy as jnp
from jax import lax
from jax.experimental import pallas as pl
from jax.experimental.pallas import tpu as pltpu
from jax.sharding import PartitionSpec as P

BLK = "blk"
N = 128
NLON = 4096
HALF = NLON // 2
ROWS = 2049
MESH = pl.DeviceIdType.MESH
BF16 = jnp.bfloat16
F32 = jnp.float32


def partner(me, step):
    z, y, x, c = lax.div(me, 32), lax.rem(lax.div(me, 8), 4), lax.rem(lax.div(me, 2), 4), lax.rem(me, 2)
    z = lax.rem(z + lax.rem(step, 4), 4)
    y = lax.rem(y + lax.rem(lax.div(step, 4), 4), 4)
    x = lax.rem(x + lax.rem(lax.div(step, 16), 4), 4)
    c = lax.rem(c + lax.div(step, 64), 2)
    return z * 32 + y * 8 + x * 2 + c


def lanes(shape, dim=1):
    return lax.broadcasted_iota(jnp.int32, shape, dim)


def arrange(group, received, swap, rows_by_source, lhs):
    for q in range(4):
        first = received[group, 32 * q : 32 * q + 16].reshape(256, 128)
        second = received[group, 32 * q + 16 : 32 * q + 32].reshape(256, 128)
        both = jnp.concatenate([first, second], axis=1)
        moved = jnp.dot(swap, both, preferred_element_type=F32).astype(BF16)
        rows_by_source[:, 32 * q : 32 * q + 16, :] = moved[:, :128].reshape(16, 16, 128)
        rows_by_source[:, 32 * q + 16 : 32 * q + 32, :] = moved[:, 128:].reshape(16, 16, 128)
    for row in range(16):
        p, h, i = row // 8, (row // 4) % 2, row % 4
        turned = rows_by_source[row].T
        for part in range(2):
            lhs[h, 64 * i : 64 * i + 64, (2 * p + part) * 128 : (2 * p + part + 1) * 128] = turned[
                64 * part : 64 * part + 64
            ]


def swap_matrix():
    row, col = lanes((256, 256), 0), lanes((256, 256), 1)
    return jnp.where(col == (row % 16) * 16 + row // 16, 1.0, 0.0).astype(BF16)


def exchange_kernel(
    leg_hbm, coef_hbm, orders_hbm, cycles_hbm,
    wave_ref, lhs_ref, basis_ref, energy_ref,
    leg, coef, orders, cycles, order_rows, cycle_cols, pick, coef_lo, coef_hi, spec,
    outgoing, incoming, by_source, lhs_first, esend, erecv,
    load_sem, send_sem, recv_sem, esend_sem, erecv_sem,
):
    me = lax.axis_index(BLK)
    small = [
        pltpu.make_async_copy(cycles_hbm, cycles, load_sem.at[8]),
        pltpu.make_async_copy(orders_hbm, orders, load_sem.at[9]),
        pltpu.make_async_copy(coef_hbm, coef, load_sem.at[10]),
    ]
    for copy in small:
        copy.start()
    big = [pltpu.make_async_copy(leg_hbm.at[:, b], leg.at[b], load_sem.at[b]) for b in range(8)]
    for copy in big:
        copy.start()

    barrier = pltpu.get_barrier_semaphore()

    def greet(step, carry):
        target = lax.rem(me + step, N)
        pl.semaphore_signal(barrier, inc=1, device_id={BLK: target}, device_id_type=MESH)
        return carry

    lax.fori_loop(1, N, greet, 0)

    small[0].wait()
    turned = cycles[...].astype(F32).T
    for b in range(8):
        cycle_cols[128 * b : 128 * b + 128, :] = jnp.broadcast_to(turned[:, b : b + 1], (128, 128))
    lane16 = lanes((16, 128)).astype(F32)

    def fill(t, carry):
        upper = cycle_cols[pl.ds(pl.multiple_of(partner(me, 2 * t) * 8, 8), 8), :]
        lower = cycle_cols[pl.ds(pl.multiple_of(partner(me, 2 * t + 1) * 8, 8), 8), :]
        wanted = jnp.concatenate([upper, lower], axis=0)
        at = pl.ds(pl.multiple_of(t * 16, 16), 16)
        for b in range(8):
            pick[at, 128 * b : 128 * b + 128] = jnp.where(wanted == lane16 + 128.0 * b, 1.0, 0.0).astype(BF16)
        return carry

    lax.fori_loop(0, N // 2, fill, 0)

    small[1].wait()
    turned = orders[...].astype(F32).T
    for b in range(2):
        order_rows[128 * b : 128 * b + 128, :] = jnp.broadcast_to(turned[:, b : b + 1], (128, 128))
    mine = [order_rows[pl.ds(2 * me + p, 1), :].astype(jnp.int32) for p in range(2)]

    small[2].wait()
    flat = coef.reshape(2 * ROWS, 128)

    def split_low(b, carry):
        turned = flat[pl.ds(pl.multiple_of(b * 128, 128), 128), :].T
        index = lanes((1, 128))
        at = pl.ds(pl.multiple_of(b * 128, 128), 128)
        for p in range(2):
            keep = jnp.where(index % 2 == p, 1.0, 0.0).astype(BF16)
            coef_lo[128 * p : 128 * p + 128, at] = turned * keep
        return carry

    def split_high(b, carry):
        turned = flat[pl.ds(pl.multiple_of(b * 128 + 2048, 128), 128), :].T
        index = lanes((1, 128))
        row = 1024 + b * 64 + index // 2
        at = pl.ds(pl.multiple_of(b * 128, 128), 128)
        for p in range(2):
            own = jnp.where(index % 2 == p, 1.0, 0.0)
            lower = jnp.where(row < ROWS - 1 - mine[p], own, 0.0)
            coef_hi[128 * p : 128 * p + 128, at] = turned * lower.astype(BF16)
            coef_hi[256 + 128 * p : 384 + 128 * p, at] = turned * (own - lower).astype(BF16)
        return carry

    lax.fori_loop(0, 16, split_low, 0)
    lax.fori_loop(0, 16, split_high, 0)
    tail = flat[2 * ROWS - 2 : 2 * ROWS, :].astype(F32)
    tail_cols = [jnp.broadcast_to(tail[p : p + 1, :], (128, 128)).T for p in range(2)]
    odd = [mine[p] % 2 == 1 for p in range(2)]

    def synthesize(q, carry):
        for b in range(2):
            pltpu.make_async_copy(leg_hbm.at[:, 0], leg.at[2 * q + b], load_sem.at[2 * q + b]).wait()
        table = [leg.at[2 * q + b].reshape(2 * ROWS, 128) for b in range(2)]
        low = jnp.concatenate([t[0:2048, :] for t in table], axis=1)
        high = jnp.concatenate([t[2048:4096, :] for t in table], axis=1)
        last = jnp.concatenate([t[4096:4098, :] for t in table], axis=1).astype(F32)
        both = jnp.dot(coef_hi[...], high, preferred_element_type=F32)
        lower = both[:256] + jnp.dot(coef_lo[...], low, preferred_element_type=F32)
        upper = both[256:]
        at = pl.ds(pl.multiple_of(q * 256, 256), 256)
        for p in range(2):
            column = jnp.concatenate([tail_cols[p], tail_cols[p]], axis=1)
            lo = lower[128 * p : 128 * p + 128]
            up = upper[128 * p : 128 * p + 128] + column * last[p : p + 1, :]
            is_odd = jnp.concatenate([odd[p], odd[p]], axis=1)
            spec[256 * p : 256 * p + 128, at] = jnp.where(is_odd, up, lo).astype(BF16)
            spec[256 * p + 128 : 256 * p + 256, at] = jnp.where(is_odd, lo, up).astype(BF16)
        return carry

    lax.fori_loop(0, 4, synthesize, 0)

    def permute(q, total):
        rows = pick[pl.ds(pl.multiple_of(q * 256, 256), 256), :]
        moved = lax.dot_general(rows, spec[...], (((1,), (1,)), ((), ())), preferred_element_type=F32)
        moved = moved.reshape(32, 8, 512)
        for g in range(2):
            quarters = [moved[:, 4 * g : 4 * g + 4, 128 * a : 128 * a + 128] for a in range(4)]
            tile = jnp.concatenate(quarters, axis=1).astype(BF16)
            outgoing[g, pl.ds(pl.multiple_of(q * 32, 32), 32)] = tile
        return total + jnp.sum(moved * moved, axis=0)

    squares = lax.fori_loop(0, 4, permute, jnp.zeros((8, 512), F32))

    part = lanes((1, 128)) // 64
    energy = jnp.zeros((1, 128), F32)
    sums = jnp.sum(squares, axis=0, keepdims=True)
    for p in range(2):
        zero_weight = jnp.where(part == 0, 1.0, 0.0)
        weight = jnp.where(mine[p] == 0, zero_weight, 2.0)
        energy += sums[:, 256 * p : 256 * p + 128] * weight
        energy += sums[:, 256 * p + 128 : 256 * p + 256] * 2.0
    energy = (energy + pltpu.roll(energy, 64, 1)) * (1.0 / 1024.0)
    esend[...] = energy
    erecv[me] = energy

    pl.semaphore_wait(barrier, N - 1)

    def send_group(g):
        def send(step, carry):
            target = partner(me, step)
            pltpu.make_async_remote_copy(
                src_ref=outgoing.at[g, step], dst_ref=incoming.at[g, me],
                send_sem=send_sem.at[g], recv_sem=recv_sem.at[g],
                device_id={BLK: target}, device_id_type=MESH,
            ).start()
            return carry

        lax.fori_loop(1, N, send, 0)
        incoming[g, me] = outgoing[g, 0]

    def send_energy(step, carry):
        pltpu.make_async_remote_copy(
            src_ref=esend, dst_ref=erecv.at[me], send_sem=esend_sem, recv_sem=erecv_sem,
            device_id={BLK: partner(me, step)}, device_id_type=MESH,
        ).start()
        return carry

    send_group(0)
    lax.fori_loop(1, N, send_energy, 0)
    send_group(1)

    lane = lanes((128, 128))
    scale = 2.0 * math.pi / NLON

    def build(a, carry):
        p, h = lax.div(a, 2), lax.rem(a, 2)
        m = order_rows[pl.ds(p, N, stride=2), :].astype(jnp.int32)
        m = jnp.where(m % 2 == h, m, ROWS - 2 - m)
        fine = ((m * lane) & (NLON - 1)).astype(F32) * scale
        coarse = ((m * (lane * 128)) & (NLON - 1)).astype(F32) * scale
        factor = jnp.where(m == 0, 1.0, 2.0)
        cos_fine, sin_fine = jnp.cos(fine), jnp.sin(fine)
        cos_coarse, sin_coarse = factor * jnp.cos(coarse), factor * jnp.sin(coarse)
        top = pl.multiple_of(p * 256, 256)
        for b in range(HALF // 128):
            c = jnp.broadcast_to(cos_coarse[:, b : b + 1], (128, 128))
            s = jnp.broadcast_to(sin_coarse[:, b : b + 1], (128, 128))
            at = slice(128 * b, 128 * b + 128)
            basis_ref[h, pl.ds(top, 128), at] = (c * cos_fine - s * sin_fine).astype(BF16)
            basis_ref[h, pl.ds(top + 128, 128), at] = (-(s * cos_fine + c * sin_fine)).astype(BF16)
        return carry

    lax.fori_loop(0, 4, build, 0)
    swap = swap_matrix()

    def arrival(g):
        return pltpu.make_async_remote_copy(
            src_ref=outgoing.at[g, pl.ds(0, N - 1)], dst_ref=incoming.at[g, pl.ds(0, N - 1)],
            send_sem=send_sem.at[g], recv_sem=recv_sem.at[g],
            device_id={BLK: partner(me, 1)}, device_id_type=MESH,
        )

    arrival(0).wait()
    arrange(0, incoming, swap, by_source, lhs_first)

    def stage(k, carry):
        low, high = synthesis(lhs_first, basis_ref, k)
        wave_ref[:, :, pl.ds(pl.multiple_of(k * 256, 256), 256)] = low
        wave_ref[:, :, pl.ds(pl.multiple_of(k * 256 + HALF, 256), 256)] = high
        return carry

    lax.fori_loop(0, HALF // 256, stage, 0)

    pltpu.make_async_remote_copy(
        src_ref=erecv.at[pl.ds(0, N - 1)], dst_ref=erecv.at[pl.ds(0, N - 1)],
        send_sem=esend_sem, recv_sem=erecv_sem,
        device_id={BLK: partner(me, 1)}, device_id_type=MESH,
    ).wait()
    energy_ref[...] = jnp.sum(erecv[...], axis=0)

    arrival(1).wait()
    arrange(1, incoming, swap, by_source, lhs_ref)


def synthesis(lhs, basis, k):
    at = pl.ds(pl.multiple_of(k * 256, 256), 256)
    even = jnp.dot(lhs[0], basis[0, :, at], preferred_element_type=F32)
    odd = jnp.dot(lhs[1], basis[1, :, at], preferred_element_type=F32)
    return (even + odd).astype(BF16).reshape(4, 64, 256), (even - odd).astype(BF16).reshape(4, 64, 256)


def finish_kernel(wave_ref, lhs_ref, basis_ref, energy_in, out_ref, energy_ref, second, sem):
    first = pltpu.make_async_copy(wave_ref, out_ref.at[0:4], sem.at[0])
    first.start()
    energy_ref[...] = energy_in[:, :64]
    copies = []
    for k in range(HALF // 256):
        low, high = synthesis(lhs_ref, basis_ref, k)
        second[:, :, 256 * k : 256 * k + 256] = low
        second[:, :, HALF + 256 * k : HALF + 256 * k + 256] = high
        if k % 2 == 1:
            for j, start in enumerate((256 * (k - 1), HALF + 256 * (k - 1))):
                at = pl.ds(start, 512)
                copy = pltpu.make_async_copy(second.at[:, :, at], out_ref.at[4:8, :, at], sem.at[1 + (k // 2) * 2 + j])
                copy.start()
                copies.append(copy)
    first.wait()
    for copy in copies:
        copy.wait()


def shards(load_coef, legendre, slab_orders, cycle_rows):
    legendre = legendre.reshape(2, ROWS, 8, 128).transpose(1, 2, 0, 3)
    load_coef = load_coef.transpose(1, 0, 2)
    hbm = pl.BlockSpec(memory_space=pltpu.HBM)
    vmem = pl.BlockSpec(memory_space=pltpu.VMEM)
    wave, lhs, basis, energy = pl.pallas_call(
        exchange_kernel,
        out_shape=(
            jax.ShapeDtypeStruct((4, 64, NLON), BF16),
            jax.ShapeDtypeStruct((2, 256, 512), BF16),
            jax.ShapeDtypeStruct((2, 512, HALF), BF16),
            jax.ShapeDtypeStruct((1, 128), F32),
        ),
        in_specs=[hbm] * 4,
        out_specs=(vmem,) * 4,
        scratch_shapes=[
            pltpu.VMEM((8, ROWS, 2, 128), BF16),
            pltpu.VMEM((ROWS, 2, 128), BF16),
            pltpu.VMEM((2, 128), jnp.int32),
            pltpu.VMEM((8, 128), jnp.int32),
            pltpu.VMEM((256, 128), F32),
            pltpu.VMEM((1024, 128), F32),
            pltpu.VMEM((1024, 1024), BF16),
            pltpu.VMEM((256, 2048), BF16),
            pltpu.VMEM((512, 2048), BF16),
            pltpu.VMEM((512, 1024), BF16),
            pltpu.VMEM((2, N, 16, 128), BF16),
            pltpu.VMEM((2, N, 16, 128), BF16),
            pltpu.VMEM((16, N, 128), BF16),
            pltpu.VMEM((2, 256, 512), BF16),
            pltpu.VMEM((1, 128), F32),
            pltpu.VMEM((N, 1, 128), F32),
            pltpu.SemaphoreType.DMA((11,)),
            pltpu.SemaphoreType.DMA((2,)),
            pltpu.SemaphoreType.DMA((2,)),
            pltpu.SemaphoreType.DMA,
            pltpu.SemaphoreType.DMA,
        ],
        name="exchange",
        compiler_params=pltpu.CompilerParams(
            collective_id=0, has_side_effects=True, vmem_limit_bytes=40 * 2**20
        ),
    )(legendre, load_coef, slab_orders.reshape(2, 128), cycle_rows.reshape(8, 128))
    potential, energy = pl.pallas_call(
        finish_kernel,
        out_shape=(
            jax.ShapeDtypeStruct((8, 64, NLON), BF16),
            jax.ShapeDtypeStruct((1, 64), F32),
        ),
        in_specs=[vmem] * 4,
        out_specs=(hbm, vmem),
        scratch_shapes=[pltpu.VMEM((4, 64, NLON), BF16), pltpu.SemaphoreType.DMA((9,))],
        name="finish",
        compiler_params=pltpu.CompilerParams(vmem_limit_bytes=40 * 2**20),
    )(wave, lhs, basis, energy)
    return potential, energy.reshape(64)


def solution(mesh):
    in_specs = (P(BLK, None, "rep"), P(BLK, None, None), P(), P())
    out_specs = (P(BLK, "rep", None), P("rep"))
    return jax.shard_map(shards, mesh=mesh, in_specs=in_specs, out_specs=out_specs, check_vma=False)
```

```python
import functools
import math

import jax
import jax.numpy as jnp
from jax import lax
from jax.experimental import pallas as pl
from jax.experimental.pallas import tpu as pltpu
from jax.sharding import PartitionSpec as P

BLK = "blk"
N = 128
NLON = 4096
HALF = NLON // 2
ROWS = 2049
MESH = pl.DeviceIdType.MESH
BF16 = jnp.bfloat16
F32 = jnp.float32


def plane(me, u):
    y, x, c = lax.rem(lax.div(me, 8), 4), lax.rem(lax.div(me, 2), 4), lax.rem(me, 2)
    y = lax.rem(y + lax.rem(u, 4), 4)
    x = lax.rem(x + lax.rem(lax.div(u, 4), 4), 4)
    c = lax.rem(c + lax.div(u, 16), 2)
    return y * 8 + x * 2 + c


def lanes(shape, dim=1):
    return lax.broadcasted_iota(jnp.int32, shape, dim)


def arrange(group, received, swap, rows_by_source, lhs):
    for q in range(4):
        first = received[group, 32 * q : 32 * q + 16].reshape(256, 128)
        second = received[group, 32 * q + 16 : 32 * q + 32].reshape(256, 128)
        both = jnp.concatenate([first, second], axis=1)
        moved = jnp.dot(swap, both, preferred_element_type=F32).astype(BF16)
        rows_by_source[:, 32 * q : 32 * q + 16, :] = moved[:, :128].reshape(16, 16, 128)
        rows_by_source[:, 32 * q + 16 : 32 * q + 32, :] = moved[:, 128:].reshape(16, 16, 128)
    for row in range(16):
        p, h, i = row // 8, (row // 4) % 2, row % 4
        turned = rows_by_source[row].T
        for part in range(2):
            lhs[h, 2 * p + part, 64 * i : 64 * i + 64, :] = turned[64 * part : 64 * part + 64]


def wide(blocks):
    return jnp.concatenate([blocks[b] for b in range(blocks.shape[0])], axis=1)


def swap_matrix():
    row, col = lanes((256, 256), 0), lanes((256, 256), 1)
    return jnp.where(col == (row % 16) * 16 + row // 16, 1.0, 0.0).astype(BF16)


def own_orders(order_rows, me):
    return [order_rows[pl.ds(2 * me + p, 1), :].astype(jnp.int32) for p in range(2)]


def exchange_kernel(
    leg_hbm, coef_hbm, orders_hbm, cycles_hbm,
    wave_ref, lhs_ref, basis_ref, energy_ref,
    leg, coef, orders, cycles, order_rows, pick, coef_lo, coef_hi, spec,
    outgoing, incoming, by_source, lhs_first, esend, erecv,
    load_sem, send_sem, recv_sem, esend_sem, erecv_sem,
):
    me = lax.axis_index(BLK)
    small = [
        pltpu.make_async_copy(cycles_hbm, cycles, load_sem.at[8]),
        pltpu.make_async_copy(orders_hbm, orders, load_sem.at[9]),
        pltpu.make_async_copy(coef_hbm, coef, load_sem.at[10]),
    ]
    for copy in small:
        copy.start()
    big = [
        pltpu.make_async_copy(leg_hbm.at[:, b], leg.at[b], load_sem.at[b]) for b in range(8)
    ]
    for copy in big:
        copy.start()

    barrier = pltpu.get_barrier_semaphore()

    def to_all(act):
        def quad(u, first):
            base = plane(me, u)
            for d in range(first, 4):
                act(base + 32 * lax.rem(lax.div(me, 32) + d, 4))

        def later(u, carry):
            quad(u, 0)
            return carry

        quad(0, 1)
        lax.fori_loop(1, 32, later, 0)

    to_all(lambda target: pl.semaphore_signal(barrier, inc=1, device_id={BLK: target}, device_id_type=MESH))
    small[0].wait()
    turned = cycles[...].astype(F32).T
    high = jnp.floor(turned * (1.0 / 128.0))
    low = turned - 128.0 * high
    lane = lanes((128, 128)).astype(F32).astype(BF16)
    none = jnp.zeros((128, 128), BF16)
    for r in range(8):
        block = jnp.broadcast_to(high[:, r : r + 1], (128, 128)).astype(BF16)
        place = jnp.broadcast_to(low[:, r : r + 1], (128, 128)).astype(BF16)
        ones = jnp.where(place == lane, jnp.ones_like(none), none)
        for b in range(8):
            pick[b, 128 * r : 128 * r + 128, :] = jnp.where(
                block == jnp.full((128, 128), b, BF16), ones, none
            )

    small[1].wait()
    turned = orders[...].astype(F32).T
    for b in range(2):
        order_rows[128 * b : 128 * b + 128, :] = jnp.broadcast_to(turned[:, b : b + 1], (128, 128))
    mine = own_orders(order_rows, me)

    small[2].wait()
    flat = coef.reshape(2 * ROWS, 128)
    index = lanes((1, 128))
    own = [jnp.where(index % 2 == p, 1.0, 0.0) for p in range(2)]
    for b in range(32):
        turned = flat[128 * b : 128 * b + 128, :].T
        for p in range(2):
            if b < 16:
                coef_lo[b, 128 * p : 128 * p + 128, :] = turned * own[p].astype(BF16)
            else:
                lower = jnp.where(64 * b + index // 2 < ROWS - 1 - mine[p], own[p], 0.0)
                coef_hi[b - 16, 128 * p : 128 * p + 128, :] = turned * lower.astype(BF16)
                coef_hi[b - 16, 256 + 128 * p : 384 + 128 * p, :] = turned * (own[p] - lower).astype(BF16)
    tail = flat[2 * ROWS - 2 : 2 * ROWS, :].astype(F32)
    tail_cols = [jnp.broadcast_to(tail[p : p + 1, :], (128, 128)).T for p in range(2)]
    odd = [mine[p] % 2 == 1 for p in range(2)]

    def synthesize(q, carry):
        for b in range(2):
            pltpu.make_async_copy(leg_hbm.at[:, 0], leg.at[2 * q + b], load_sem.at[2 * q + b]).wait()
        table = [leg.at[2 * q + b].reshape(2 * ROWS, 128) for b in range(2)]
        low = jnp.concatenate([t[0:2048, :] for t in table], axis=1)
        high = jnp.concatenate([t[2048:4096, :] for t in table], axis=1)
        last = jnp.concatenate([t[4096:4098, :] for t in table], axis=1).astype(F32)
        both = jnp.dot(wide(coef_hi), high, preferred_element_type=F32)
        lower = both[:256] + jnp.dot(wide(coef_lo), low, preferred_element_type=F32)
        upper = both[256:]
        for p in range(2):
            column = jnp.concatenate([tail_cols[p]] * 2, axis=1)
            lo = lower[128 * p : 128 * p + 128]
            up = upper[128 * p : 128 * p + 128] + column * last[p : p + 1, :]
            is_odd = jnp.concatenate([odd[p]] * 2, axis=1)
            even, other = jnp.where(is_odd, up, lo).astype(BF16), jnp.where(is_odd, lo, up).astype(BF16)
            for b in range(2):
                spec[2 * q + b, 256 * p : 256 * p + 128, :] = even[:, 128 * b : 128 * b + 128]
                spec[2 * q + b, 256 * p + 128 : 256 * p + 256, :] = other[:, 128 * b : 128 * b + 128]
        return carry

    lax.fori_loop(0, 4, synthesize, 0)

    def send_one(g, target):
        pltpu.make_async_remote_copy(
            src_ref=outgoing.at[g, target], dst_ref=incoming.at[g, me],
            send_sem=send_sem.at[g], recv_sem=recv_sem.at[g],
            device_id={BLK: target}, device_id_type=MESH,
        ).start()

    squares = jnp.zeros((8, 512), F32)
    for d in (2, 3, 1, 0):
        z = lax.rem(lax.div(me, 32) + d, 4)
        at = pl.ds(pl.multiple_of(z * 256, 256), 256)
        rows = jnp.concatenate([pick[b, at, :] for b in range(8)], axis=1)
        moved = lax.dot_general(rows, wide(spec), (((1,), (1,)), ((), ())), preferred_element_type=F32)
        moved = moved.reshape(32, 8, 512)
        for g in range(2):
            quarters = [moved[:, 4 * g : 4 * g + 4, 128 * a : 128 * a + 128] for a in range(4)]
            tile = jnp.concatenate(quarters, axis=1).astype(BF16)
            outgoing[g, pl.ds(pl.multiple_of(z * 32, 32), 32)] = tile
        squares += jnp.sum(moved * moved, axis=0)
        if d == 2:
            pl.semaphore_wait(barrier, N - 1)

        def plane_sends(u, carry):
            send_one(0, plane(me, u) + 32 * z)
            return carry

        lax.fori_loop(0 if d else 1, 32, plane_sends, 0)
    incoming[0, me] = outgoing[0, me]

    part = lanes((1, 128)) // 64
    energy = jnp.zeros((1, 128), F32)
    sums = jnp.sum(squares, axis=0, keepdims=True)
    for p in range(2):
        zero_weight = jnp.where(part == 0, 1.0, 0.0)
        weight = jnp.where(mine[p] == 0, zero_weight, 2.0)
        energy += sums[:, 256 * p : 256 * p + 128] * weight
        energy += sums[:, 256 * p + 128 : 256 * p + 256] * 2.0
    energy = (energy + pltpu.roll(energy, 64, 1)) * (1.0 / 1024.0)
    esend[...] = energy
    erecv[me] = energy

    def send_energy(target):
        pltpu.make_async_remote_copy(
            src_ref=esend, dst_ref=erecv.at[me], send_sem=esend_sem, recv_sem=erecv_sem,
            device_id={BLK: target}, device_id_type=MESH,
        ).start()

    to_all(send_energy)
    to_all(functools.partial(send_one, 1))
    incoming[1, me] = outgoing[1, me]

    lane = lanes((128, 128))
    scale = 2.0 * math.pi / NLON

    def build(a, carry):
        p, h = lax.div(a, 2), lax.rem(a, 2)
        m = order_rows[pl.ds(p, N, stride=2), :].astype(jnp.int32)
        m = jnp.where(m % 2 == h, m, ROWS - 2 - m)
        fine = ((m * lane) & (NLON - 1)).astype(F32) * scale
        coarse = ((m * (lane * 128)) & (NLON - 1)).astype(F32) * scale
        factor = jnp.where(m == 0, 1.0, 2.0)
        cos_fine, sin_fine = jnp.cos(fine), jnp.sin(fine)
        cos_coarse, sin_coarse = factor * jnp.cos(coarse), factor * jnp.sin(coarse)
        top = pl.multiple_of(p * 256, 256)
        for b in range(HALF // 128):
            c = jnp.broadcast_to(cos_coarse[:, b : b + 1], (128, 128))
            s = jnp.broadcast_to(sin_coarse[:, b : b + 1], (128, 128))
            basis_ref[h, b, pl.ds(top, 128), :] = (c * cos_fine - s * sin_fine).astype(BF16)
            basis_ref[h, b, pl.ds(top + 128, 128), :] = (-(s * cos_fine + c * sin_fine)).astype(BF16)
        return carry

    lax.fori_loop(0, 4, build, 0)
    swap = swap_matrix()

    def arrival(g):
        return pltpu.make_async_remote_copy(
            src_ref=outgoing.at[g, pl.ds(0, N - 1)], dst_ref=incoming.at[g, pl.ds(0, N - 1)],
            send_sem=send_sem.at[g], recv_sem=recv_sem.at[g],
            device_id={BLK: lax.rem(me + 1, N)}, device_id_type=MESH,
        )

    arrival(0).wait()
    arrange(0, incoming, swap, by_source, lhs_first)

    def stage(k, carry):
        low, high = synthesis(lhs_first, basis_ref, k)
        wave_ref[:, :, pl.ds(pl.multiple_of(k * 256, 256), 256)] = low
        wave_ref[:, :, pl.ds(pl.multiple_of(k * 256 + HALF, 256), 256)] = high
        return carry

    lax.fori_loop(0, HALF // 256, stage, 0)

    pltpu.make_async_remote_copy(
        src_ref=erecv.at[pl.ds(0, N - 1)], dst_ref=erecv.at[pl.ds(0, N - 1)],
        send_sem=esend_sem, recv_sem=erecv_sem,
        device_id={BLK: lax.rem(me + 1, N)}, device_id_type=MESH,
    ).wait()
    energy_ref[...] = jnp.sum(erecv[...], axis=0)

    arrival(1).wait()
    arrange(1, incoming, swap, by_source, lhs_ref)


def synthesis(lhs, basis, k):
    even, odd = (
        jnp.dot(
            wide(lhs.at[h]),
            jnp.concatenate([basis[h, 2 * k], basis[h, 2 * k + 1]], axis=1),
            preferred_element_type=F32,
        )
        for h in range(2)
    )
    return (even + odd).astype(BF16).reshape(4, 64, 256), (even - odd).astype(BF16).reshape(4, 64, 256)


def finish_kernel(wave_ref, lhs_ref, basis_ref, energy_in, out_ref, energy_ref, second, sem):
    first = pltpu.make_async_copy(wave_ref, out_ref.at[0:4], sem.at[0])
    first.start()
    energy_ref[...] = energy_in[:, :64]
    copies = []
    for k in range(HALF // 256):
        low, high = synthesis(lhs_ref, basis_ref, k)
        second[:, :, 256 * k : 256 * k + 256] = low
        second[:, :, HALF + 256 * k : HALF + 256 * k + 256] = high
        if k % 2 == 1:
            for j, start in enumerate((256 * (k - 1), HALF + 256 * (k - 1))):
                at = pl.ds(start, 512)
                copy = pltpu.make_async_copy(second.at[:, :, at], out_ref.at[4:8, :, at], sem.at[1 + (k // 2) * 2 + j])
                copy.start()
                copies.append(copy)
    first.wait()
    for copy in copies:
        copy.wait()


def shards(load_coef, legendre, slab_orders, cycle_rows):
    legendre = legendre.reshape(2, ROWS, 8, 128).transpose(1, 2, 0, 3)
    load_coef = load_coef.transpose(1, 0, 2)
    hbm = pl.BlockSpec(memory_space=pltpu.HBM)
    vmem = pl.BlockSpec(memory_space=pltpu.VMEM)
    operands = (legendre, load_coef, slab_orders.reshape(2, 128), cycle_rows.reshape(8, 128))
    wave, lhs, basis, energy = pl.pallas_call(
        exchange_kernel,
        out_shape=(
            jax.ShapeDtypeStruct((4, 64, NLON), BF16),
            jax.ShapeDtypeStruct((2, 4, 256, 128), BF16),
            jax.ShapeDtypeStruct((2, HALF // 128, 512, 128), BF16),
            jax.ShapeDtypeStruct((1, 128), F32),
        ),
        in_specs=[hbm] * 4,
        out_specs=(vmem,) * 4,
        scratch_shapes=[
            pltpu.VMEM((8, ROWS, 2, 128), BF16),
            pltpu.VMEM((ROWS, 2, 128), BF16),
            pltpu.VMEM((2, 128), jnp.int32),
            pltpu.VMEM((8, 128), jnp.int32),
            pltpu.VMEM((256, 128), F32),
            pltpu.VMEM((8, 1024, 128), BF16),
            pltpu.VMEM((16, 256, 128), BF16),
            pltpu.VMEM((16, 512, 128), BF16),
            pltpu.VMEM((8, 512, 128), BF16),
            pltpu.VMEM((2, N, 16, 128), BF16),
            pltpu.VMEM((2, N, 16, 128), BF16),
            pltpu.VMEM((16, N, 128), BF16),
            pltpu.VMEM((2, 4, 256, 128), BF16),
            pltpu.VMEM((1, 128), F32),
            pltpu.VMEM((N, 1, 128), F32),
            pltpu.SemaphoreType.DMA((11,)),
            pltpu.SemaphoreType.DMA((2,)),
            pltpu.SemaphoreType.DMA((2,)),
            pltpu.SemaphoreType.DMA,
            pltpu.SemaphoreType.DMA,
        ],
        name="exchange",
        compiler_params=pltpu.CompilerParams(
            collective_id=0, has_side_effects=True, vmem_limit_bytes=40 * 2**20
        ),
    )(*[pltpu.with_memory_space_constraint(value, pltpu.HBM) for value in operands])
    potential, energy = pl.pallas_call(
        finish_kernel,
        out_shape=(
            jax.ShapeDtypeStruct((8, 64, NLON), BF16),
            jax.ShapeDtypeStruct((1, 64), F32),
        ),
        in_specs=[vmem] * 4,
        out_specs=(hbm, vmem),
        scratch_shapes=[pltpu.VMEM((4, 64, NLON), BF16), pltpu.SemaphoreType.DMA((9,))],
        name="finish",
        compiler_params=pltpu.CompilerParams(vmem_limit_bytes=24 * 2**20),
    )(wave, lhs, basis, energy)
    return potential, energy.reshape(64)


def solution(mesh):
    in_specs = (P(BLK, None, "rep"), P(BLK, None, None), P(), P())
    out_specs = (P(BLK, "rep", None), P("rep"))
    return jax.shard_map(shards, mesh=mesh, in_specs=in_specs, out_specs=out_specs, check_vma=False)
```

```python
import functools
import math

import jax
import jax.numpy as jnp
from jax import lax
from jax.experimental import pallas as pl
from jax.experimental.pallas import tpu as pltpu
from jax.sharding import PartitionSpec as P

BLK = "blk"
N = 128
NLON = 4096
HALF = NLON // 2
ROWS = 2049
MESH = pl.DeviceIdType.MESH
BF16 = jnp.bfloat16
F32 = jnp.float32


def plane(me, u):
    y, x, c = lax.rem(lax.div(me, 8), 4), lax.rem(lax.div(me, 2), 4), lax.rem(me, 2)
    y = lax.rem(y + lax.rem(u, 4), 4)
    x = lax.rem(x + lax.rem(lax.div(u, 4), 4), 4)
    c = lax.rem(c + lax.div(u, 16), 2)
    return y * 8 + x * 2 + c


def lanes(shape, dim=1):
    return lax.broadcasted_iota(jnp.int32, shape, dim)


def arrange(group, received, swap, rows_by_source, lhs):
    for q in range(4):
        first = received[group, 32 * q : 32 * q + 16].reshape(256, 128)
        second = received[group, 32 * q + 16 : 32 * q + 32].reshape(256, 128)
        both = jnp.concatenate([first, second], axis=1)
        moved = jnp.dot(swap, both, preferred_element_type=F32).astype(BF16)
        rows_by_source[:, 32 * q : 32 * q + 16, :] = moved[:, :128].reshape(16, 16, 128)
        rows_by_source[:, 32 * q + 16 : 32 * q + 32, :] = moved[:, 128:].reshape(16, 16, 128)
    for row in range(16):
        p, h, i = row // 8, (row // 4) % 2, row % 4
        turned = rows_by_source[row].T
        for part in range(2):
            lhs[h, 2 * p + part, 64 * i : 64 * i + 64, :] = turned[64 * part : 64 * part + 64]


def wide(blocks):
    return jnp.concatenate([blocks[b] for b in range(blocks.shape[0])], axis=1)


def swap_matrix():
    row, col = lanes((256, 256), 0), lanes((256, 256), 1)
    return jnp.where(col == (row % 16) * 16 + row // 16, 1.0, 0.0).astype(BF16)


def own_orders(order_rows, me):
    return [order_rows[pl.ds(2 * me + p, 1), :].astype(jnp.int32) for p in range(2)]


def exchange_kernel(
    leg_hbm, coef_hbm, orders_hbm, cycles_hbm,
    wave_ref, lhs_ref, basis_ref, energy_ref,
    leg, coef, orders, cycles, order_rows, pick, coef_lo, coef_hi, spec,
    outgoing, incoming, by_source, lhs_first, esend, ecolumn, eplane,
    load_sem, send_sem, recv_sem, esend_sem, erecv_sem,
):
    me = lax.axis_index(BLK)
    small = [
        pltpu.make_async_copy(cycles_hbm, cycles, load_sem.at[8]),
        pltpu.make_async_copy(orders_hbm, orders, load_sem.at[9]),
        pltpu.make_async_copy(coef_hbm, coef, load_sem.at[10]),
    ]
    for copy in small:
        copy.start()
    big = [
        pltpu.make_async_copy(leg_hbm.at[:, b], leg.at[b], load_sem.at[b]) for b in range(8)
    ]
    for copy in big:
        copy.start()

    barrier = pltpu.get_barrier_semaphore()

    def to_all(act):
        def quad(u, first):
            base = plane(me, u)
            for d in range(first, 4):
                act(base + 32 * lax.rem(lax.div(me, 32) + d, 4))

        def later(u, carry):
            quad(u, 0)
            return carry

        quad(0, 1)
        lax.fori_loop(1, 32, later, 0)

    to_all(lambda target: pl.semaphore_signal(barrier, inc=1, device_id={BLK: target}, device_id_type=MESH))
    small[1].wait()
    turned = orders[...].astype(F32).T
    for b in range(2):
        order_rows[128 * b : 128 * b + 128, :] = jnp.broadcast_to(turned[:, b : b + 1], (128, 128))
    mine = own_orders(order_rows, me)

    small[2].wait()
    flat = coef.reshape(2 * ROWS, 128)
    index = lanes((1, 128))
    own = [jnp.where(index % 2 == p, 1.0, 0.0) for p in range(2)]
    for b in range(32):
        turned = flat[128 * b : 128 * b + 128, :].T
        for p in range(2):
            if b < 16:
                coef_lo[b, 128 * p : 128 * p + 128, :] = turned * own[p].astype(BF16)
            else:
                lower = jnp.where(64 * b + index // 2 < ROWS - 1 - mine[p], own[p], 0.0)
                coef_hi[b - 16, 128 * p : 128 * p + 128, :] = turned * lower.astype(BF16)
                coef_hi[b - 16, 256 + 128 * p : 384 + 128 * p, :] = turned * (own[p] - lower).astype(BF16)
    tail = flat[2 * ROWS - 2 : 2 * ROWS, :].astype(F32)
    tail_cols = [jnp.broadcast_to(tail[p : p + 1, :], (128, 128)).T for p in range(2)]
    odd = [mine[p] % 2 == 1 for p in range(2)]

    small[0].wait()
    lane = lanes((128, 128)).astype(F32).astype(BF16)
    none = jnp.zeros((128, 128), BF16)
    one = jnp.ones((128, 128), BF16)

    def fill(r):
        wanted = jnp.broadcast_to(cycles[pl.ds(r, 1), :].astype(F32), (128, 128)).T
        high = jnp.floor(wanted * (1.0 / 128.0))
        ones = jnp.where((wanted - 128.0 * high).astype(BF16) == lane, one, none)
        block = high.astype(BF16)
        for b in range(8):
            pick[b, pl.ds(pl.multiple_of(r * 128, 128), 128), :] = jnp.where(
                block == jnp.full((128, 128), b, BF16), ones, none
            )

    def synthesize(q, carry):
        for b in range(2):
            pltpu.make_async_copy(leg_hbm.at[:, 0], leg.at[2 * q + b], load_sem.at[2 * q + b]).wait()
        table = [leg.at[2 * q + b].reshape(2 * ROWS, 128) for b in range(2)]
        low = jnp.concatenate([t[0:2048, :] for t in table], axis=1)
        high = jnp.concatenate([t[2048:4096, :] for t in table], axis=1)
        last = jnp.concatenate([t[4096:4098, :] for t in table], axis=1).astype(F32)
        both = jnp.dot(wide(coef_hi), high, preferred_element_type=F32)
        lower = both[:256] + jnp.dot(wide(coef_lo), low, preferred_element_type=F32)
        upper = both[256:]
        for p in range(2):
            column = jnp.concatenate([tail_cols[p]] * 2, axis=1)
            lo = lower[128 * p : 128 * p + 128]
            up = upper[128 * p : 128 * p + 128] + column * last[p : p + 1, :]
            is_odd = jnp.concatenate([odd[p]] * 2, axis=1)
            even, other = jnp.where(is_odd, up, lo).astype(BF16), jnp.where(is_odd, lo, up).astype(BF16)
            for b in range(2):
                spec[2 * q + b, 256 * p : 256 * p + 128, :] = even[:, 128 * b : 128 * b + 128]
                spec[2 * q + b, 256 * p + 128 : 256 * p + 256, :] = other[:, 128 * b : 128 * b + 128]
        for j in range(2):
            fill(2 * q + j)
        return carry

    lax.fori_loop(0, 4, synthesize, 0)

    def send_one(g, target):
        pltpu.make_async_remote_copy(
            src_ref=outgoing.at[g, target], dst_ref=incoming.at[g, me],
            send_sem=send_sem.at[g], recv_sem=recv_sem.at[g],
            device_id={BLK: target}, device_id_type=MESH,
        ).start()

    squares = jnp.zeros((8, 512), F32)
    for d in (2, 3, 1, 0):
        z = lax.rem(lax.div(me, 32) + d, 4)
        at = pl.ds(pl.multiple_of(z * 256, 256), 256)
        rows = jnp.concatenate([pick[b, at, :] for b in range(8)], axis=1)
        moved = lax.dot_general(rows, wide(spec), (((1,), (1,)), ((), ())), preferred_element_type=F32)
        moved = moved.reshape(32, 8, 512)
        for g in range(2):
            quarters = [moved[:, 4 * g : 4 * g + 4, 128 * a : 128 * a + 128] for a in range(4)]
            tile = jnp.concatenate(quarters, axis=1).astype(BF16)
            outgoing[g, pl.ds(pl.multiple_of(z * 32, 32), 32)] = tile
        squares += jnp.sum(moved * moved, axis=0)
        if d == 2:
            pl.semaphore_wait(barrier, N - 1)

        def plane_sends(u, carry):
            send_one(0, plane(me, u) + 32 * z)
            return carry

        lax.fori_loop(0 if d else 1, 32, plane_sends, 0)
    incoming[0, me] = outgoing[0, me]

    part = lanes((1, 128)) // 64
    energy = jnp.zeros((1, 128), F32)
    sums = jnp.sum(squares, axis=0, keepdims=True)
    for p in range(2):
        zero_weight = jnp.where(part == 0, 1.0, 0.0)
        weight = jnp.where(mine[p] == 0, zero_weight, 2.0)
        energy += sums[:, 256 * p : 256 * p + 128] * weight
        energy += sums[:, 256 * p + 128 : 256 * p + 256] * 2.0
    energy = (energy + pltpu.roll(energy, 64, 1)) * (1.0 / 1024.0)
    mine_z, mine_u = lax.div(me, 32), lax.rem(me, 32)
    esend[0] = energy
    ecolumn[mine_z] = energy

    def send_energy(stage, target, slot):
        pltpu.make_async_remote_copy(
            src_ref=esend.at[stage], dst_ref=slot, send_sem=esend_sem.at[stage], recv_sem=erecv_sem.at[stage],
            device_id={BLK: target}, device_id_type=MESH,
        ).start()

    def energy_arrival(stage, slots, count):
        pltpu.make_async_remote_copy(
            src_ref=slots.at[pl.ds(0, count)], dst_ref=slots.at[pl.ds(0, count)],
            send_sem=esend_sem.at[stage], recv_sem=erecv_sem.at[stage],
            device_id={BLK: lax.rem(me + 1, N)}, device_id_type=MESH,
        ).wait()

    for d in range(1, 4):
        send_energy(0, mine_u + 32 * lax.rem(mine_z + d, 4), ecolumn.at[mine_z])
    to_all(functools.partial(send_one, 1))
    incoming[1, me] = outgoing[1, me]

    lane = lanes((128, 128))
    scale = 2.0 * math.pi / NLON

    def build(a, carry):
        p, h = lax.div(a, 2), lax.rem(a, 2)
        m = order_rows[pl.ds(p, N, stride=2), :].astype(jnp.int32)
        m = jnp.where(m % 2 == h, m, ROWS - 2 - m)
        fine = ((m * lane) & (NLON - 1)).astype(F32) * scale
        coarse = ((m * (lane * 128)) & (NLON - 1)).astype(F32) * scale
        factor = jnp.where(m == 0, 1.0, 2.0)
        cos_fine, sin_fine = jnp.cos(fine), jnp.sin(fine)
        cos_coarse, sin_coarse = factor * jnp.cos(coarse), factor * jnp.sin(coarse)
        top = pl.multiple_of(p * 256, 256)
        for b in range(HALF // 128):
            c = jnp.broadcast_to(cos_coarse[:, b : b + 1], (128, 128))
            s = jnp.broadcast_to(sin_coarse[:, b : b + 1], (128, 128))
            basis_ref[h, b, pl.ds(top, 128), :] = (c * cos_fine - s * sin_fine).astype(BF16)
            basis_ref[h, b, pl.ds(top + 128, 128), :] = (-(s * cos_fine + c * sin_fine)).astype(BF16)
        return carry

    lax.fori_loop(0, 4, build, 0)
    swap = swap_matrix()

    def arrival(g):
        return pltpu.make_async_remote_copy(
            src_ref=outgoing.at[g, pl.ds(0, N - 1)], dst_ref=incoming.at[g, pl.ds(0, N - 1)],
            send_sem=send_sem.at[g], recv_sem=recv_sem.at[g],
            device_id={BLK: lax.rem(me + 1, N)}, device_id_type=MESH,
        )

    energy_arrival(0, ecolumn, 3)
    partial = jnp.sum(ecolumn[...], axis=0)
    esend[1] = partial
    eplane[mine_u] = partial

    arrival(0).wait()
    arrange(0, incoming, swap, by_source, lhs_first)

    def stage(k, carry):
        low, high = synthesis(lhs_first, basis_ref, k)
        wave_ref[:, :, pl.ds(pl.multiple_of(k * 256, 256), 256)] = low
        wave_ref[:, :, pl.ds(pl.multiple_of(k * 256 + HALF, 256), 256)] = high
        return carry

    def plane_energy(u, carry):
        send_energy(1, plane(me, u) + 32 * mine_z, eplane.at[mine_u])
        return carry

    lax.fori_loop(1, 32, plane_energy, 0)
    lax.fori_loop(0, HALF // 256, stage, 0)
    energy_arrival(1, eplane, 31)
    energy_ref[...] = jnp.sum(eplane[...], axis=0)
    arrival(1).wait()
    arrange(1, incoming, swap, by_source, lhs_ref)


def synthesis(lhs, basis, k):
    even, odd = (
        jnp.dot(
            wide(lhs.at[h]),
            jnp.concatenate([basis[h, 2 * k], basis[h, 2 * k + 1]], axis=1),
            preferred_element_type=F32,
        )
        for h in range(2)
    )
    return (even + odd).astype(BF16).reshape(4, 64, 256), (even - odd).astype(BF16).reshape(4, 64, 256)


def finish_kernel(wave_ref, lhs_ref, basis_ref, energy_in, out_ref, energy_ref, second, sem):
    first = pltpu.make_async_copy(wave_ref, out_ref.at[0:4], sem.at[0])
    first.start()
    energy_ref[...] = energy_in[:, :64]

    def store(k, half):
        at = pl.ds(pl.multiple_of(k * 512 + HALF * half, 512), 512)
        return pltpu.make_async_copy(second.at[:, :, at], out_ref.at[4:8, :, at], sem.at[1 + 2 * k + half])

    def stage(k, carry):
        for j in range(2):
            low, high = synthesis(lhs_ref, basis_ref, 2 * k + j)
            second[:, :, pl.ds(pl.multiple_of(k * 512 + 256 * j, 256), 256)] = low
            second[:, :, pl.ds(pl.multiple_of(k * 512 + 256 * j + HALF, 256), 256)] = high
        store(k, 0).start()
        store(k, 1).start()
        return carry

    lax.fori_loop(0, 4, stage, 0)
    first.wait()
    for k in range(4):
        store(k, 0).wait()
        store(k, 1).wait()


def shards(load_coef, legendre, slab_orders, cycle_rows):
    legendre = legendre.reshape(2, ROWS, 8, 128).transpose(1, 2, 0, 3)
    load_coef = load_coef.transpose(1, 0, 2)
    hbm = pl.BlockSpec(memory_space=pltpu.HBM)
    vmem = pl.BlockSpec(memory_space=pltpu.VMEM)
    operands = (legendre, load_coef, slab_orders.reshape(2, 128), cycle_rows.reshape(8, 128))
    wave, lhs, basis, energy = pl.pallas_call(
        exchange_kernel,
        out_shape=(
            jax.ShapeDtypeStruct((4, 64, NLON), BF16),
            jax.ShapeDtypeStruct((2, 4, 256, 128), BF16),
            jax.ShapeDtypeStruct((2, HALF // 128, 512, 128), BF16),
            jax.ShapeDtypeStruct((1, 128), F32),
        ),
        in_specs=[hbm] * 4,
        out_specs=(vmem,) * 4,
        scratch_shapes=[
            pltpu.VMEM((8, ROWS, 2, 128), BF16),
            pltpu.VMEM((ROWS, 2, 128), BF16),
            pltpu.VMEM((2, 128), jnp.int32),
            pltpu.VMEM((8, 128), jnp.int32),
            pltpu.VMEM((256, 128), F32),
            pltpu.VMEM((8, 1024, 128), BF16),
            pltpu.VMEM((16, 256, 128), BF16),
            pltpu.VMEM((16, 512, 128), BF16),
            pltpu.VMEM((8, 512, 128), BF16),
            pltpu.VMEM((2, N, 16, 128), BF16),
            pltpu.VMEM((2, N, 16, 128), BF16),
            pltpu.VMEM((16, N, 128), BF16),
            pltpu.VMEM((2, 4, 256, 128), BF16),
            pltpu.VMEM((2, 1, 128), F32),
            pltpu.VMEM((4, 1, 128), F32),
            pltpu.VMEM((32, 1, 128), F32),
            pltpu.SemaphoreType.DMA((11,)),
            pltpu.SemaphoreType.DMA((2,)),
            pltpu.SemaphoreType.DMA((2,)),
            pltpu.SemaphoreType.DMA((2,)),
            pltpu.SemaphoreType.DMA((2,)),
        ],
        name="exchange",
        compiler_params=pltpu.CompilerParams(
            collective_id=0, has_side_effects=True, vmem_limit_bytes=40 * 2**20
        ),
    )(*[pltpu.with_memory_space_constraint(value, pltpu.HBM) for value in operands])
    potential, energy = pl.pallas_call(
        finish_kernel,
        out_shape=(
            jax.ShapeDtypeStruct((8, 64, NLON), BF16),
            jax.ShapeDtypeStruct((1, 64), F32),
        ),
        in_specs=[vmem] * 4,
        out_specs=(hbm, vmem),
        scratch_shapes=[pltpu.VMEM((4, 64, NLON), BF16), pltpu.SemaphoreType.DMA((9,))],
        name="finish",
        compiler_params=pltpu.CompilerParams(vmem_limit_bytes=24 * 2**20),
    )(wave, lhs, basis, energy)
    return potential, energy.reshape(64)


def solution(mesh):
    in_specs = (P(BLK, None, "rep"), P(BLK, None, None), P(), P())
    out_specs = (P(BLK, "rep", None), P("rep"))
    return jax.shard_map(shards, mesh=mesh, in_specs=in_specs, out_specs=out_specs, check_vma=False)
```

```python
import functools
import math

import jax
import jax.numpy as jnp
from jax import lax
from jax.experimental import pallas as pl
from jax.experimental.pallas import tpu as pltpu
from jax.sharding import PartitionSpec as P

BLK = "blk"
N = 128
NLON = 4096
HALF = NLON // 2
ROWS = 2049
MESH = pl.DeviceIdType.MESH
BF16 = jnp.bfloat16
F32 = jnp.float32


def plane(me, u):
    y, x, c = lax.rem(lax.div(me, 8), 4), lax.rem(lax.div(me, 2), 4), lax.rem(me, 2)
    y = lax.rem(y + lax.rem(u, 4), 4)
    x = lax.rem(x + lax.rem(lax.div(u, 4), 4), 4)
    c = lax.rem(c + lax.div(u, 16), 2)
    return y * 8 + x * 2 + c


def lanes(shape, dim=1):
    return lax.broadcasted_iota(jnp.int32, shape, dim)


def arrange(group, received, swap, rows_by_source, lhs):
    for q in range(4):
        first = received[group, 32 * q : 32 * q + 16].reshape(256, 128)
        second = received[group, 32 * q + 16 : 32 * q + 32].reshape(256, 128)
        both = jnp.concatenate([first, second], axis=1)
        moved = jnp.dot(swap, both, preferred_element_type=F32).astype(BF16)
        rows_by_source[:, 32 * q : 32 * q + 16, :] = moved[:, :128].reshape(16, 16, 128)
        rows_by_source[:, 32 * q + 16 : 32 * q + 32, :] = moved[:, 128:].reshape(16, 16, 128)
    for row in range(16):
        p, h, i = row // 8, (row // 4) % 2, row % 4
        turned = rows_by_source[row].T
        for part in range(2):
            lhs[h, 2 * p + part, 64 * i : 64 * i + 64, :] = turned[64 * part : 64 * part + 64]


def wide(blocks):
    return jnp.concatenate([blocks[b] for b in range(blocks.shape[0])], axis=1)


def swap_matrix():
    row, col = lanes((256, 256), 0), lanes((256, 256), 1)
    return jnp.where(col == (row % 16) * 16 + row // 16, 1.0, 0.0).astype(BF16)


def own_orders(order_rows, me):
    return [order_rows[pl.ds(2 * me + p, 1), :].astype(jnp.int32) for p in range(2)]


def exchange_kernel(
    leg_hbm, coef_hbm, orders_hbm, cycles_hbm,
    wave_ref, lhs_ref, basis_ref, energy_ref,
    leg, coef, orders, cycles, order_rows, pick, coef_lo, coef_hi, spec,
    outgoing, incoming, by_source, lhs_first, esend, ecolumn, eplane,
    load_sem, send_sem, recv_sem, esend_sem, erecv_sem,
):
    me = lax.axis_index(BLK)
    small = [
        pltpu.make_async_copy(cycles_hbm, cycles, load_sem.at[8]),
        pltpu.make_async_copy(orders_hbm, orders, load_sem.at[9]),
        pltpu.make_async_copy(coef_hbm, coef, load_sem.at[10]),
    ]
    for copy in small:
        copy.start()
    big = [
        pltpu.make_async_copy(leg_hbm.at[:, b], leg.at[b], load_sem.at[b]) for b in range(8)
    ]
    for copy in big:
        copy.start()

    barrier = pltpu.get_barrier_semaphore()

    def to_all(act):
        def quad(u, first):
            base = plane(me, u)
            for d in range(first, 4):
                act(base + 32 * lax.rem(lax.div(me, 32) + d, 4))

        def later(u, carry):
            quad(u, 0)
            return carry

        quad(0, 1)
        lax.fori_loop(1, 32, later, 0)

    to_all(lambda target: pl.semaphore_signal(barrier, inc=1, device_id={BLK: target}, device_id_type=MESH))
    small[1].wait()
    turned = orders[...].astype(F32).T
    for b in range(2):
        order_rows[128 * b : 128 * b + 128, :] = jnp.broadcast_to(turned[:, b : b + 1], (128, 128))
    mine = own_orders(order_rows, me)

    small[2].wait()
    flat = coef.reshape(2 * ROWS, 128)
    index = lanes((1, 128))
    for p in range(2):
        for b in range(16):
            turned = flat[pl.ds(256 * b + p, 128, stride=2), :].T
            if b < 8:
                coef_lo[p, b] = turned
            else:
                lower = jnp.where(128 * b + index < ROWS - 1 - mine[p], 1.0, 0.0)
                coef_hi[p, b - 8, 0:128, :] = turned * lower.astype(BF16)
                coef_hi[p, b - 8, 128:256, :] = turned * (1.0 - lower).astype(BF16)
    tail = flat[2 * ROWS - 2 : 2 * ROWS, :].astype(F32)
    tail_cols = [jnp.broadcast_to(tail[p : p + 1, :], (128, 128)).T for p in range(2)]
    odd = [mine[p] % 2 == 1 for p in range(2)]

    small[0].wait()
    lane = lanes((128, 128)).astype(F32).astype(BF16)
    none = jnp.zeros((128, 128), BF16)
    one = jnp.ones((128, 128), BF16)

    def fill(r):
        wanted = jnp.broadcast_to(cycles[pl.ds(r, 1), :].astype(F32), (128, 128)).T
        high = jnp.floor(wanted * (1.0 / 128.0))
        ones = jnp.where((wanted - 128.0 * high).astype(BF16) == lane, one, none)
        block = high.astype(BF16)
        for b in range(8):
            pick[b, pl.ds(pl.multiple_of(r * 128, 128), 128), :] = jnp.where(
                block == jnp.full((128, 128), b, BF16), ones, none
            )

    def synthesize(q, carry):
        for b in range(4):
            pltpu.make_async_copy(leg_hbm.at[:, 0], leg.at[4 * q + b], load_sem.at[4 * q + b]).wait()
        table = [leg.at[4 * q + b].reshape(2 * ROWS, 128) for b in range(4)]
        last = jnp.concatenate([t[4096:4098, :] for t in table], axis=1).astype(F32)
        for p in range(2):
            low = jnp.concatenate([t[pl.ds(p, 1024, stride=2), :] for t in table], axis=1)
            high = jnp.concatenate([t[pl.ds(2048 + p, 1024, stride=2), :] for t in table], axis=1)
            both = jnp.dot(wide(coef_hi.at[p]), high, preferred_element_type=F32)
            lo = both[:128] + jnp.dot(wide(coef_lo.at[p]), low, preferred_element_type=F32)
            column = jnp.concatenate([tail_cols[p]] * 4, axis=1)
            up = both[128:] + column * last[p : p + 1, :]
            is_odd = jnp.concatenate([odd[p]] * 4, axis=1)
            even, other = jnp.where(is_odd, up, lo).astype(BF16), jnp.where(is_odd, lo, up).astype(BF16)
            for b in range(4):
                spec[4 * q + b, 256 * p : 256 * p + 128, :] = even[:, 128 * b : 128 * b + 128]
                spec[4 * q + b, 256 * p + 128 : 256 * p + 256, :] = other[:, 128 * b : 128 * b + 128]
        for j in range(4):
            fill(4 * q + j)
        return carry

    lax.fori_loop(0, 2, synthesize, 0)

    def send_one(g, target):
        pltpu.make_async_remote_copy(
            src_ref=outgoing.at[g, target], dst_ref=incoming.at[g, me],
            send_sem=send_sem.at[g], recv_sem=recv_sem.at[g],
            device_id={BLK: target}, device_id_type=MESH,
        ).start()

    squares = jnp.zeros((8, 512), F32)
    for d in (2, 3, 1, 0):
        z = lax.rem(lax.div(me, 32) + d, 4)
        at = pl.ds(pl.multiple_of(z * 256, 256), 256)
        rows = jnp.concatenate([pick[b, at, :] for b in range(8)], axis=1)
        moved = lax.dot_general(rows, wide(spec), (((1,), (1,)), ((), ())), preferred_element_type=F32)
        moved = moved.reshape(32, 8, 512)
        for g in range(2):
            quarters = [moved[:, 4 * g : 4 * g + 4, 128 * a : 128 * a + 128] for a in range(4)]
            tile = jnp.concatenate(quarters, axis=1).astype(BF16)
            outgoing[g, pl.ds(pl.multiple_of(z * 32, 32), 32)] = tile
        squares += jnp.sum(moved * moved, axis=0)
        if d == 2:
            pl.semaphore_wait(barrier, N - 1)

        def plane_sends(u, carry):
            send_one(0, plane(me, u) + 32 * z)
            return carry

        lax.fori_loop(0 if d else 1, 32, plane_sends, 0)
    incoming[0, me] = outgoing[0, me]

    part = lanes((1, 128)) // 64
    energy = jnp.zeros((1, 128), F32)
    sums = jnp.sum(squares, axis=0, keepdims=True)
    for p in range(2):
        zero_weight = jnp.where(part == 0, 1.0, 0.0)
        weight = jnp.where(mine[p] == 0, zero_weight, 2.0)
        energy += sums[:, 256 * p : 256 * p + 128] * weight
        energy += sums[:, 256 * p + 128 : 256 * p + 256] * 2.0
    energy = (energy + pltpu.roll(energy, 64, 1)) * (1.0 / 1024.0)
    mine_z, mine_u = lax.div(me, 32), lax.rem(me, 32)
    esend[0] = energy
    ecolumn[mine_z] = energy

    def send_energy(stage, target, slot):
        pltpu.make_async_remote_copy(
            src_ref=esend.at[stage], dst_ref=slot, send_sem=esend_sem.at[stage], recv_sem=erecv_sem.at[stage],
            device_id={BLK: target}, device_id_type=MESH,
        ).start()

    def energy_arrival(stage, slots, count):
        pltpu.make_async_remote_copy(
            src_ref=slots.at[pl.ds(0, count)], dst_ref=slots.at[pl.ds(0, count)],
            send_sem=esend_sem.at[stage], recv_sem=erecv_sem.at[stage],
            device_id={BLK: lax.rem(me + 1, N)}, device_id_type=MESH,
        ).wait()

    for d in range(1, 4):
        send_energy(0, mine_u + 32 * lax.rem(mine_z + d, 4), ecolumn.at[mine_z])
    to_all(functools.partial(send_one, 1))
    incoming[1, me] = outgoing[1, me]

    lane = lanes((128, 128))
    scale = 2.0 * math.pi / NLON

    def build(a, carry):
        p, h = lax.div(a, 2), lax.rem(a, 2)
        m = order_rows[pl.ds(p, N, stride=2), :].astype(jnp.int32)
        m = jnp.where(m % 2 == h, m, ROWS - 2 - m)
        fine = ((m * lane) & (NLON - 1)).astype(F32) * scale
        coarse = ((m * (lane * 128)) & (NLON - 1)).astype(F32) * scale
        factor = jnp.where(m == 0, 1.0, 2.0)
        cos_fine, sin_fine = jnp.cos(fine), jnp.sin(fine)
        cos_coarse, sin_coarse = factor * jnp.cos(coarse), factor * jnp.sin(coarse)
        top = pl.multiple_of(p * 256, 256)
        for b in range(HALF // 128):
            c = jnp.broadcast_to(cos_coarse[:, b : b + 1], (128, 128))
            s = jnp.broadcast_to(sin_coarse[:, b : b + 1], (128, 128))
            basis_ref[h, b, pl.ds(top, 128), :] = (c * cos_fine - s * sin_fine).astype(BF16)
            basis_ref[h, b, pl.ds(top + 128, 128), :] = (-(s * cos_fine + c * sin_fine)).astype(BF16)
        return carry

    lax.fori_loop(0, 4, build, 0)
    swap = swap_matrix()

    def arrival(g):
        return pltpu.make_async_remote_copy(
            src_ref=outgoing.at[g, pl.ds(0, N - 1)], dst_ref=incoming.at[g, pl.ds(0, N - 1)],
            send_sem=send_sem.at[g], recv_sem=recv_sem.at[g],
            device_id={BLK: lax.rem(me + 1, N)}, device_id_type=MESH,
        )

    energy_arrival(0, ecolumn, 3)
    partial = jnp.sum(ecolumn[...], axis=0)
    esend[1] = partial
    eplane[mine_u] = partial

    arrival(0).wait()
    arrange(0, incoming, swap, by_source, lhs_first)

    def stage(k, carry):
        low, high = synthesis(lhs_first, basis_ref, k)
        wave_ref[:, :, pl.ds(pl.multiple_of(k * 256, 256), 256)] = low
        wave_ref[:, :, pl.ds(pl.multiple_of(k * 256 + HALF, 256), 256)] = high
        return carry

    def plane_energy(u, carry):
        send_energy(1, plane(me, u) + 32 * mine_z, eplane.at[mine_u])
        return carry

    lax.fori_loop(1, 32, plane_energy, 0)
    lax.fori_loop(0, HALF // 256, stage, 0)
    energy_arrival(1, eplane, 31)
    energy_ref[...] = jnp.sum(eplane[...], axis=0)
    arrival(1).wait()
    arrange(1, incoming, swap, by_source, lhs_ref)


def synthesis(lhs, basis, k):
    even, odd = (
        jnp.dot(
            wide(lhs.at[h]),
            jnp.concatenate([basis[h, 2 * k], basis[h, 2 * k + 1]], axis=1),
            preferred_element_type=F32,
        )
        for h in range(2)
    )
    return (even + odd).astype(BF16).reshape(4, 64, 256), (even - odd).astype(BF16).reshape(4, 64, 256)


def finish_kernel(wave_ref, lhs_ref, basis_ref, energy_in, out_ref, energy_ref, second, energy, sem):
    energy[...] = energy_in[:, :64]
    copies = [
        pltpu.make_async_copy(wave_ref, out_ref.at[0:4], sem.at[0]),
        pltpu.make_async_copy(energy, energy_ref, sem.at[9]),
    ]
    for copy in copies:
        copy.start()
    for k in range(HALF // 256):
        low, high = synthesis(lhs_ref, basis_ref, k)
        second[:, :, 256 * k : 256 * k + 256] = low
        second[:, :, HALF + 256 * k : HALF + 256 * k + 256] = high
        if k % 2 == 1:
            for j, start in enumerate((256 * (k - 1), HALF + 256 * (k - 1))):
                at = pl.ds(start, 512)
                copy = pltpu.make_async_copy(second.at[:, :, at], out_ref.at[4:8, :, at], sem.at[k + j])
                copy.start()
                copies.append(copy)
    for copy in copies:
        copy.wait()


def shards(load_coef, legendre, slab_orders, cycle_rows):
    legendre = legendre.reshape(2, ROWS, 8, 128).transpose(1, 2, 0, 3)
    load_coef = load_coef.transpose(1, 0, 2)
    hbm = pl.BlockSpec(memory_space=pltpu.HBM)
    vmem = pl.BlockSpec(memory_space=pltpu.VMEM)
    operands = (legendre, load_coef, slab_orders.reshape(2, 128), cycle_rows.reshape(8, 128))
    wave, lhs, basis, energy = pl.pallas_call(
        exchange_kernel,
        out_shape=(
            jax.ShapeDtypeStruct((4, 64, NLON), BF16),
            jax.ShapeDtypeStruct((2, 4, 256, 128), BF16),
            jax.ShapeDtypeStruct((2, HALF // 128, 512, 128), BF16),
            jax.ShapeDtypeStruct((1, 128), F32),
        ),
        in_specs=[hbm] * 4,
        out_specs=(vmem,) * 4,
        scratch_shapes=[
            pltpu.VMEM((8, ROWS, 2, 128), BF16),
            pltpu.VMEM((ROWS, 2, 128), BF16),
            pltpu.VMEM((2, 128), jnp.int32),
            pltpu.VMEM((8, 128), jnp.int32),
            pltpu.VMEM((256, 128), F32),
            pltpu.VMEM((8, 1024, 128), BF16),
            pltpu.VMEM((2, 8, 128, 128), BF16),
            pltpu.VMEM((2, 8, 256, 128), BF16),
            pltpu.VMEM((8, 512, 128), BF16),
            pltpu.VMEM((2, N, 16, 128), BF16),
            pltpu.VMEM((2, N, 16, 128), BF16),
            pltpu.VMEM((16, N, 128), BF16),
            pltpu.VMEM((2, 4, 256, 128), BF16),
            pltpu.VMEM((2, 1, 128), F32),
            pltpu.VMEM((4, 1, 128), F32),
            pltpu.VMEM((32, 1, 128), F32),
            pltpu.SemaphoreType.DMA((11,)),
            pltpu.SemaphoreType.DMA((2,)),
            pltpu.SemaphoreType.DMA((2,)),
            pltpu.SemaphoreType.DMA((2,)),
            pltpu.SemaphoreType.DMA((2,)),
        ],
        name="exchange",
        compiler_params=pltpu.CompilerParams(
            collective_id=0, has_side_effects=True, vmem_limit_bytes=40 * 2**20
        ),
    )(*[pltpu.with_memory_space_constraint(value, pltpu.HBM) for value in operands])
    potential, energy = pl.pallas_call(
        finish_kernel,
        out_shape=(
            jax.ShapeDtypeStruct((8, 64, NLON), BF16),
            jax.ShapeDtypeStruct((1, 64), F32),
        ),
        in_specs=[vmem] * 4,
        out_specs=(hbm, hbm),
        scratch_shapes=[
            pltpu.VMEM((4, 64, NLON), BF16),
            pltpu.VMEM((1, 64), F32),
            pltpu.SemaphoreType.DMA((10,)),
        ],
        name="finish",
        compiler_params=pltpu.CompilerParams(vmem_limit_bytes=24 * 2**20),
    )(wave, lhs, basis, energy)
    return potential, energy.reshape(64)


def solution(mesh):
    in_specs = (P(BLK, None, "rep"), P(BLK, None, None), P(), P())
    out_specs = (P(BLK, "rep", None), P("rep"))
    return jax.shard_map(shards, mesh=mesh, in_specs=in_specs, out_specs=out_specs, check_vma=False)
```

```python
import functools
import math

import jax
import jax.numpy as jnp
from jax import lax
from jax.experimental import pallas as pl
from jax.experimental.pallas import tpu as pltpu
from jax.sharding import PartitionSpec as P

BLK = "blk"
N = 128
NLON = 4096
HALF = NLON // 2
ROWS = 2049
MESH = pl.DeviceIdType.MESH
BF16 = jnp.bfloat16
F32 = jnp.float32


def plane(me, u):
    y, x, c = lax.rem(lax.div(me, 8), 4), lax.rem(lax.div(me, 2), 4), lax.rem(me, 2)
    y = lax.rem(y + lax.rem(u, 4), 4)
    x = lax.rem(x + lax.rem(lax.div(u, 4), 4), 4)
    c = lax.rem(c + lax.div(u, 16), 2)
    return y * 8 + x * 2 + c


def lanes(shape, dim=1):
    return lax.broadcasted_iota(jnp.int32, shape, dim)


def arrange(group, received, swap, rows_by_source, lhs):
    for q in range(4):
        first = received[group, 32 * q : 32 * q + 16].reshape(256, 128)
        second = received[group, 32 * q + 16 : 32 * q + 32].reshape(256, 128)
        both = jnp.concatenate([first, second], axis=1)
        moved = jnp.dot(swap, both, preferred_element_type=F32).astype(BF16)
        rows_by_source[:, 32 * q : 32 * q + 16, :] = moved[:, :128].reshape(16, 16, 128)
        rows_by_source[:, 32 * q + 16 : 32 * q + 32, :] = moved[:, 128:].reshape(16, 16, 128)
    for row in range(16):
        p, h, i = row // 8, (row // 4) % 2, row % 4
        turned = rows_by_source[row].T
        for part in range(2):
            lhs[h, 2 * p + part, 64 * i : 64 * i + 64, :] = turned[64 * part : 64 * part + 64]


def wide(blocks):
    return jnp.concatenate([blocks[b] for b in range(blocks.shape[0])], axis=1)


def swap_matrix():
    row, col = lanes((256, 256), 0), lanes((256, 256), 1)
    return jnp.where(col == (row % 16) * 16 + row // 16, 1.0, 0.0).astype(BF16)


def own_orders(order_rows, me):
    return [order_rows[pl.ds(2 * me + p, 1), :].astype(jnp.int32) for p in range(2)]


def exchange_kernel(
    leg_hbm, coef_hbm, orders_hbm, cycles_hbm,
    wave_ref, lhs_ref, basis_ref, energy_ref,
    leg, coef, orders, cycles, order_rows, pick, coef_lo, coef_hi, spec,
    outgoing, incoming, by_source, lhs_first, esend, ecolumn, eplane,
    load_sem, send_sem, recv_sem, esend_sem, erecv_sem,
):
    me = lax.axis_index(BLK)
    small = [
        pltpu.make_async_copy(cycles_hbm, cycles, load_sem.at[8]),
        pltpu.make_async_copy(orders_hbm, orders, load_sem.at[9]),
        pltpu.make_async_copy(coef_hbm, coef, load_sem.at[10]),
    ]
    for copy in small:
        copy.start()
    big = [
        pltpu.make_async_copy(leg_hbm.at[:, b], leg.at[b], load_sem.at[b]) for b in range(8)
    ]
    for copy in big:
        copy.start()

    barrier = pltpu.get_barrier_semaphore()

    def to_all(act):
        def quad(u, first):
            base = plane(me, u)
            for d in range(first, 4):
                act(base + 32 * lax.rem(lax.div(me, 32) + d, 4))

        def later(u, carry):
            quad(u, 0)
            return carry

        quad(0, 1)
        lax.fori_loop(1, 32, later, 0)

    to_all(lambda target: pl.semaphore_signal(barrier, inc=1, device_id={BLK: target}, device_id_type=MESH))
    small[1].wait()
    turned = orders[...].astype(F32).T
    for b in range(2):
        order_rows[128 * b : 128 * b + 128, :] = jnp.broadcast_to(turned[:, b : b + 1], (128, 128))
    mine = own_orders(order_rows, me)

    small[2].wait()
    flat = coef.reshape(2 * ROWS, 128)
    index = lanes((1, 128))
    for p in range(2):
        for b in range(16):
            turned = flat[pl.ds(256 * b + p, 128, stride=2), :].T
            if b < 8:
                coef_lo[p, b] = turned
            else:
                lower = jnp.where(128 * b + index < ROWS - 1 - mine[p], 1.0, 0.0)
                coef_hi[p, b - 8, 0:128, :] = turned * lower.astype(BF16)
                coef_hi[p, b - 8, 128:256, :] = turned * (1.0 - lower).astype(BF16)
    tail = flat[2 * ROWS - 2 : 2 * ROWS, :].astype(F32)
    tail_cols = [jnp.broadcast_to(tail[p : p + 1, :], (128, 128)).T for p in range(2)]
    odd = [mine[p] % 2 == 1 for p in range(2)]

    small[0].wait()
    lane = lanes((128, 128)).astype(F32).astype(BF16)
    none = jnp.zeros((128, 128), BF16)
    one = jnp.ones((128, 128), BF16)

    def fill(r):
        wanted = jnp.broadcast_to(cycles[pl.ds(r, 1), :].astype(F32), (128, 128)).T
        high = jnp.floor(wanted * (1.0 / 128.0))
        ones = jnp.where((wanted - 128.0 * high).astype(BF16) == lane, one, none)
        block = high.astype(BF16)
        for b in range(8):
            pick[b, pl.ds(pl.multiple_of(r * 128, 128), 128), :] = jnp.where(
                block == jnp.full((128, 128), b, BF16), ones, none
            )

    def synthesize(q, carry):
        for b in range(4):
            pltpu.make_async_copy(leg_hbm.at[:, 0], leg.at[4 * q + b], load_sem.at[4 * q + b]).wait()
        table = [leg.at[4 * q + b].reshape(2 * ROWS, 128) for b in range(4)]
        last = jnp.concatenate([t[4096:4098, :] for t in table], axis=1).astype(F32)
        for p in range(2):
            low = jnp.concatenate([t[pl.ds(p, 1024, stride=2), :] for t in table], axis=1)
            high = jnp.concatenate([t[pl.ds(2048 + p, 1024, stride=2), :] for t in table], axis=1)
            both = jnp.dot(wide(coef_hi.at[p]), high, preferred_element_type=F32)
            lo = both[:128] + jnp.dot(wide(coef_lo.at[p]), low, preferred_element_type=F32)
            column = jnp.concatenate([tail_cols[p]] * 4, axis=1)
            up = both[128:] + column * last[p : p + 1, :]
            is_odd = jnp.concatenate([odd[p]] * 4, axis=1)
            even, other = jnp.where(is_odd, up, lo).astype(BF16), jnp.where(is_odd, lo, up).astype(BF16)
            for b in range(4):
                spec[4 * q + b, 256 * p : 256 * p + 128, :] = even[:, 128 * b : 128 * b + 128]
                spec[4 * q + b, 256 * p + 128 : 256 * p + 256, :] = other[:, 128 * b : 128 * b + 128]
        for j in range(4):
            fill(4 * q + j)
        return carry

    lax.fori_loop(0, 2, synthesize, 0)

    def send_one(g, target):
        pltpu.make_async_remote_copy(
            src_ref=outgoing.at[g, target], dst_ref=incoming.at[g, me],
            send_sem=send_sem.at[g], recv_sem=recv_sem.at[g],
            device_id={BLK: target}, device_id_type=MESH,
        ).start()

    squares = jnp.zeros((8, 512), F32)
    for d in (2, 3, 1, 0):
        z = lax.rem(lax.div(me, 32) + d, 4)
        at = pl.ds(pl.multiple_of(z * 256, 256), 256)
        rows = jnp.concatenate([pick[b, at, :] for b in range(8)], axis=1)
        moved = lax.dot_general(rows, wide(spec), (((1,), (1,)), ((), ())), preferred_element_type=F32)
        moved = moved.reshape(32, 8, 512)
        for g in range(2):
            quarters = [moved[:, 4 * g : 4 * g + 4, 128 * a : 128 * a + 128] for a in range(4)]
            tile = jnp.concatenate(quarters, axis=1).astype(BF16)
            outgoing[g, pl.ds(pl.multiple_of(z * 32, 32), 32)] = tile
        squares += jnp.sum(moved * moved, axis=0)
        if d == 2:
            pl.semaphore_wait(barrier, N - 1)

        def plane_sends(u, carry):
            send_one(0, plane(me, u) + 32 * z)
            return carry

        lax.fori_loop(0 if d else 1, 32, plane_sends, 0)
    incoming[0, me] = outgoing[0, me]

    part = lanes((1, 128)) // 64
    energy = jnp.zeros((1, 128), F32)
    sums = jnp.sum(squares, axis=0, keepdims=True)
    for p in range(2):
        zero_weight = jnp.where(part == 0, 1.0, 0.0)
        weight = jnp.where(mine[p] == 0, zero_weight, 2.0)
        energy += sums[:, 256 * p : 256 * p + 128] * weight
        energy += sums[:, 256 * p + 128 : 256 * p + 256] * 2.0
    energy = (energy + pltpu.roll(energy, 64, 1)) * (1.0 / 1024.0)
    mine_z, mine_u = lax.div(me, 32), lax.rem(me, 32)
    esend[0] = energy
    ecolumn[mine_z] = energy

    def send_energy(stage, target, slot):
        pltpu.make_async_remote_copy(
            src_ref=esend.at[stage], dst_ref=slot, send_sem=esend_sem.at[stage], recv_sem=erecv_sem.at[stage],
            device_id={BLK: target}, device_id_type=MESH,
        ).start()

    def energy_arrival(stage, slots, count):
        pltpu.make_async_remote_copy(
            src_ref=slots.at[pl.ds(0, count)], dst_ref=slots.at[pl.ds(0, count)],
            send_sem=esend_sem.at[stage], recv_sem=erecv_sem.at[stage],
            device_id={BLK: lax.rem(me + 1, N)}, device_id_type=MESH,
        ).wait()

    for d in range(1, 4):
        send_energy(0, mine_u + 32 * lax.rem(mine_z + d, 4), ecolumn.at[mine_z])
    for d in (2, 3, 1, 0):
        z = lax.rem(mine_z + d, 4)

        def second_sends(u, carry, z=z):
            send_one(1, plane(me, u) + 32 * z)
            return carry

        lax.fori_loop(0 if d else 1, 32, second_sends, 0)
    incoming[1, me] = outgoing[1, me]

    lane = lanes((128, 128))
    scale = 2.0 * math.pi / NLON

    def build(a, carry):
        p, h = lax.div(a, 2), lax.rem(a, 2)
        m = order_rows[pl.ds(p, N, stride=2), :].astype(jnp.int32)
        m = jnp.where(m % 2 == h, m, ROWS - 2 - m)
        fine = ((m * lane) & (NLON - 1)).astype(F32) * scale
        coarse = ((m * (lane * 128)) & (NLON - 1)).astype(F32) * scale
        factor = jnp.where(m == 0, 1.0, 2.0)
        cos_fine, sin_fine = jnp.cos(fine), jnp.sin(fine)
        cos_coarse, sin_coarse = factor * jnp.cos(coarse), factor * jnp.sin(coarse)
        top = pl.multiple_of(p * 256, 256)
        for b in range(HALF // 128):
            c = jnp.broadcast_to(cos_coarse[:, b : b + 1], (128, 128))
            s = jnp.broadcast_to(sin_coarse[:, b : b + 1], (128, 128))
            basis_ref[h, b, pl.ds(top, 128), :] = (c * cos_fine - s * sin_fine).astype(BF16)
            basis_ref[h, b, pl.ds(top + 128, 128), :] = (-(s * cos_fine + c * sin_fine)).astype(BF16)
        return carry

    lax.fori_loop(0, 4, build, 0)
    swap = swap_matrix()

    def arrival(g):
        return pltpu.make_async_remote_copy(
            src_ref=outgoing.at[g, pl.ds(0, N - 1)], dst_ref=incoming.at[g, pl.ds(0, N - 1)],
            send_sem=send_sem.at[g], recv_sem=recv_sem.at[g],
            device_id={BLK: lax.rem(me + 1, N)}, device_id_type=MESH,
        )

    energy_arrival(0, ecolumn, 3)
    partial = jnp.sum(ecolumn[...], axis=0)
    esend[1] = partial
    eplane[mine_u] = partial

    arrival(0).wait()
    arrange(0, incoming, swap, by_source, lhs_first)

    def stage(k, carry):
        low, high = synthesis(lhs_first, basis_ref, k)
        wave_ref[:, :, pl.ds(pl.multiple_of(k * 256, 256), 256)] = low
        wave_ref[:, :, pl.ds(pl.multiple_of(k * 256 + HALF, 256), 256)] = high
        return carry

    def plane_energy(u, carry):
        send_energy(1, plane(me, u) + 32 * mine_z, eplane.at[mine_u])
        return carry

    lax.fori_loop(1, 32, plane_energy, 0)
    lax.fori_loop(0, HALF // 256, stage, 0)
    energy_arrival(1, eplane, 31)
    energy_ref[...] = jnp.sum(eplane[...], axis=0)
    arrival(1).wait()
    arrange(1, incoming, swap, by_source, lhs_ref)


def synthesis(lhs, basis, k):
    even, odd = (
        jnp.dot(
            wide(lhs.at[h]),
            jnp.concatenate([basis[h, 2 * k], basis[h, 2 * k + 1]], axis=1),
            preferred_element_type=F32,
        )
        for h in range(2)
    )
    return (even + odd).astype(BF16).reshape(4, 64, 256), (even - odd).astype(BF16).reshape(4, 64, 256)


def finish_kernel(wave_ref, lhs_ref, basis_ref, energy_in, out_ref, energy_ref, second, energy, sem):
    energy[...] = energy_in[:, :64]
    copies = [
        pltpu.make_async_copy(wave_ref, out_ref.at[0:4], sem.at[0]),
        pltpu.make_async_copy(energy, energy_ref, sem.at[9]),
    ]
    for copy in copies:
        copy.start()
    for k in range(HALF // 256):
        low, high = synthesis(lhs_ref, basis_ref, k)
        second[:, :, 256 * k : 256 * k + 256] = low
        second[:, :, HALF + 256 * k : HALF + 256 * k + 256] = high
        if k % 2 == 1:
            for j, start in enumerate((256 * (k - 1), HALF + 256 * (k - 1))):
                at = pl.ds(start, 512)
                copy = pltpu.make_async_copy(second.at[:, :, at], out_ref.at[4:8, :, at], sem.at[k + j])
                copy.start()
                copies.append(copy)
    for copy in copies:
        copy.wait()


def shards(load_coef, legendre, slab_orders, cycle_rows):
    legendre = legendre.reshape(2, ROWS, 8, 128).transpose(1, 2, 0, 3)
    load_coef = load_coef.transpose(1, 0, 2)
    hbm = pl.BlockSpec(memory_space=pltpu.HBM)
    vmem = pl.BlockSpec(memory_space=pltpu.VMEM)
    operands = (legendre, load_coef, slab_orders.reshape(2, 128), cycle_rows.reshape(8, 128))
    wave, lhs, basis, energy = pl.pallas_call(
        exchange_kernel,
        out_shape=(
            jax.ShapeDtypeStruct((4, 64, NLON), BF16),
            jax.ShapeDtypeStruct((2, 4, 256, 128), BF16),
            jax.ShapeDtypeStruct((2, HALF // 128, 512, 128), BF16),
            jax.ShapeDtypeStruct((1, 128), F32),
        ),
        in_specs=[hbm] * 4,
        out_specs=(vmem,) * 4,
        scratch_shapes=[
            pltpu.VMEM((8, ROWS, 2, 128), BF16),
            pltpu.VMEM((ROWS, 2, 128), BF16),
            pltpu.VMEM((2, 128), jnp.int32),
            pltpu.VMEM((8, 128), jnp.int32),
            pltpu.VMEM((256, 128), F32),
            pltpu.VMEM((8, 1024, 128), BF16),
            pltpu.VMEM((2, 8, 128, 128), BF16),
            pltpu.VMEM((2, 8, 256, 128), BF16),
            pltpu.VMEM((8, 512, 128), BF16),
            pltpu.VMEM((2, N, 16, 128), BF16),
            pltpu.VMEM((2, N, 16, 128), BF16),
            pltpu.VMEM((16, N, 128), BF16),
            pltpu.VMEM((2, 4, 256, 128), BF16),
            pltpu.VMEM((2, 1, 128), F32),
            pltpu.VMEM((4, 1, 128), F32),
            pltpu.VMEM((32, 1, 128), F32),
            pltpu.SemaphoreType.DMA((11,)),
            pltpu.SemaphoreType.DMA((2,)),
            pltpu.SemaphoreType.DMA((2,)),
            pltpu.SemaphoreType.DMA((2,)),
            pltpu.SemaphoreType.DMA((2,)),
        ],
        name="exchange",
        compiler_params=pltpu.CompilerParams(
            collective_id=0, has_side_effects=True, vmem_limit_bytes=40 * 2**20
        ),
    )(*[pltpu.with_memory_space_constraint(value, pltpu.HBM) for value in operands])
    potential, energy = pl.pallas_call(
        finish_kernel,
        out_shape=(
            jax.ShapeDtypeStruct((8, 64, NLON), BF16),
            jax.ShapeDtypeStruct((1, 64), F32),
        ),
        in_specs=[vmem] * 4,
        out_specs=(hbm, hbm),
        scratch_shapes=[
            pltpu.VMEM((4, 64, NLON), BF16),
            pltpu.VMEM((1, 64), F32),
            pltpu.SemaphoreType.DMA((10,)),
        ],
        name="finish",
        compiler_params=pltpu.CompilerParams(vmem_limit_bytes=24 * 2**20),
    )(wave, lhs, basis, energy)
    return potential, energy.reshape(64)


def solution(mesh):
    in_specs = (P(BLK, None, "rep"), P(BLK, None, None), P(), P())
    out_specs = (P(BLK, "rep", None), P("rep"))
    return jax.shard_map(shards, mesh=mesh, in_specs=in_specs, out_specs=out_specs, check_vma=False)
```
